32 devices in a mesh: groups: 2 (over y), ffn: 4 (over x, core), width: 4 (over z).
Axes of the slice: x: 2, y: 2, z: 4, core: 2. Of those that a mesh axis runs over, the one named last changes fastest.
Arguments:
- hidden: bfloat16 [2048, 8192], P(('groups', 'ffn'), 'width'), parts along dimension 0, may hold values from -8.4 to 8.4
- upstream: bfloat16 [2048, 8192], P(('groups', 'ffn'), 'width'), parts along dimension 0, may hold values from -6 to 6
- query_frozen_weight: bfloat16 [8192, 8192], P('width', 'ffn'), may hold values from -0.0625 to 0.0625
- key_value_frozen_weight: bfloat16 [2, 8192, 1024], P(None, 'width', 'ffn'), may hold values from -0.0625 to 0.0625
- output_frozen_weight: bfloat16 [8192, 8192], P('ffn', 'width'), may hold values from -0.0625 to 0.0625
- adapter_down: bfloat16 [6, 16, 8192], P('groups', None, 'width'), parts along dimension 0, may hold values from -0.0625 to 0.0625
- query_up_map: bfloat16 [32, 8192], P('groups', 'ffn'), parts along dimension 0, may hold values from -0.0625 to 0.0625
- key_value_up_maps: bfloat16 [4, 16, 1024], P('groups', None, 'ffn'), parts along dimension 0, may hold values from -0.0625 to 0.0625
- output_down_map: bfloat16 [32, 8192], P('groups', 'ffn'), parts along dimension 0, may hold values from -0.0625 to 0.0625
- output_up: bfloat16 [32, 8192], P('groups', 'width'), parts along dimension 0, may hold values from -0.0625 to 0.0625
Outputs:
- hidden_gradient: bfloat16 [2048, 8192], P(('groups', 'ffn'), 'width'), parts along dimension 0
- down_map_gradient: float32 [6, 16, 8192], P('groups', None, 'width'), parts along dimension 0
- query_up_map_gradient: float32 [32, 8192], P('groups', 'ffn'), parts along dimension 0
- key_value_up_maps_gradient: float32 [4, 16, 1024], P('groups', None, 'ffn'), parts along dimension 0
- output_down_map_gradient: float32 [32, 8192], P('groups', 'ffn'), parts along dimension 0
- output_up_map_gradient: float32 [32, 8192], P('groups', 'width'), parts along dimension 0
The draws below stay inside these ranges and needn't reach their ends.
There are 2 independent parts, one for each index of `groups`. The reference program is written for one: setup_inputs(seed, part) draws one part's arguments, and reference() takes and returns one part's arrays. A program takes and returns all parts, laid end to end along the dimension named above; an argument that names none is the same for every part. Nothing has to cross between parts.
All inputs are finite; a program needn't handle non-finite values.
Results may differ from the reference program's by a relative error of at most 0.04.
Values may be sent and summed in bfloat16 or wider, within the bound.
A program may use at most 128 MiB of HBM per device.

```python
import math
import jax
import jax.numpy as jnp
from jax import lax

MODEL_WIDTH = 8192
HEADS = 64
KV_HEADS = 8
HEAD_DIM = 128
ADAPTER_RANK = 16
TOKENS = 1024
N_FFN = 4
N_WIDTH = 4


def draw_hidden(key, part):
    base_key = jax.random.fold_in(jax.random.fold_in(key, 11), 0)
    values = jnp.clip(jax.random.normal(base_key, (TOKENS, MODEL_WIDTH), jnp.float32), -6.0, 6.0)
    return values.astype(jnp.bfloat16)


def steps_of(rng, dims, cuts, smallest, top_value):
    level = 1.0
    for dim, blocks in cuts:
        draws = jax.random.uniform(jax.random.fold_in(jax.random.fold_in(rng, 6), dim), (blocks,), jnp.float32, smallest / len(cuts), top_value / len(cuts))
        level = level * jnp.repeat(jnp.exp(draws), dims[dim] // blocks).reshape((-1,) + (1,) * (len(dims) - 1 - dim))
    return level


def normal_values(own_key, dims, scale, bound, cuts=(), held_as=jnp.bfloat16):
    drawn = scale * jax.random.normal(own_key, dims, jnp.float32)
    if cuts:
        drawn = drawn * steps_of(own_key, dims, cuts, -0.22, 0.18)
    return jnp.clip(drawn, -bound, bound).astype(held_as)


def setup_inputs(seed: int = 0, part: int = 0) -> dict:
    splits = jax.random.split(jax.random.key(seed), 11)
    own_keys = jax.random.split(jax.random.fold_in(splits[10], part), 11)
    return {
        "hidden": draw_hidden(jax.random.fold_in(jax.random.fold_in(splits[10], part), 71), part),
        "upstream": normal_values(own_keys[1], (TOKENS, MODEL_WIDTH), 1.0, 6.0, ((0, 4), (1, 4))),
        "query_frozen_weight": normal_values(splits[2], (MODEL_WIDTH, HEADS * HEAD_DIM), MODEL_WIDTH ** -0.5, 0.0625, ((0, 4), (1, 4))),
        "key_value_frozen_weight": normal_values(splits[3], (2, MODEL_WIDTH, KV_HEADS * HEAD_DIM), MODEL_WIDTH ** -0.5, 0.0625, ((1, 4), (2, 4))),
        "output_frozen_weight": normal_values(splits[4], (HEADS * HEAD_DIM, MODEL_WIDTH), (HEADS * HEAD_DIM) ** -0.5, 0.0625, ((0, 4), (1, 4))),
        "adapter_down": normal_values(own_keys[5], (3, ADAPTER_RANK, MODEL_WIDTH), MODEL_WIDTH ** -0.5, 0.0625, ((2, 4),)),
        "query_up_map": normal_values(own_keys[6], (ADAPTER_RANK, HEADS * HEAD_DIM), MODEL_WIDTH ** -0.5, 0.0625, ((1, 4),)),
        "key_value_up_maps": normal_values(own_keys[7], (2, ADAPTER_RANK, KV_HEADS * HEAD_DIM), MODEL_WIDTH ** -0.5, 0.0625, ((2, 4),)),
        "output_down_map": normal_values(own_keys[8], (ADAPTER_RANK, HEADS * HEAD_DIM), (HEADS * HEAD_DIM) ** -0.5, 0.0625, ((1, 4),)),
        "output_up": normal_values(own_keys[9], (ADAPTER_RANK, MODEL_WIDTH), MODEL_WIDTH ** -0.5, 0.0625, ((1, 4),)),
    }


adapter_scale = 2.0
rope_base = 500000.0

def rotate(values, positions, first_dim, direction):
    columns = values.shape[1]
    head_dims = (first_dim + jnp.arange(columns, dtype=jnp.int32)) % HEAD_DIM
    pair_dims = head_dims - head_dims % 2
    frequency = jnp.exp(pair_dims.astype(jnp.float32) * (-math.log(rope_base) / HEAD_DIM))
    angles = positions.astype(jnp.float32)[:, None] * frequency[None, :]
    is_even = head_dims % 2 == 0
    following = jnp.roll(values, -1, axis=1)
    preceding = jnp.roll(values, 1, axis=1)
    partner = jnp.where(is_even[None, :], -following, preceding)
    return values * jnp.cos(angles) + direction * partner * jnp.sin(angles)

def width_grouped(left_side, right_side):
    block_size = left_side.shape[1] // N_WIDTH
    running = jnp.zeros((left_side.shape[0], right_side.shape[1]), jnp.float32)
    for block_index in range(N_WIDTH):
        offset = block_index * block_size
        partial_value = jnp.dot(left_side[:, offset:offset + block_size], right_side[offset:offset + block_size, :], preferred_element_type=jnp.float32)
        running = running + lax.optimization_barrier(partial_value.astype(jnp.bfloat16)).astype(jnp.float32)
    return running

def head_grouped(contraction_pairs, token_count):
    running = jnp.zeros((token_count, MODEL_WIDTH), jnp.float32)
    for block_index in range(N_FFN):
        partial_value = jnp.zeros((token_count, MODEL_WIDTH), jnp.float32)
        for gradient, weight in contraction_pairs:
            block_size = weight.shape[1] // N_FFN
            offset = block_index * block_size
            partial_value = partial_value + jnp.dot(gradient[:, offset:offset + block_size], weight[:, offset:offset + block_size].T, preferred_element_type=jnp.float32)
        running = running + lax.optimization_barrier(partial_value.astype(jnp.bfloat16)).astype(jnp.float32)
    return running

def reference(hidden, upstream, query_frozen_weight, key_value_frozen_weight, output_frozen_weight, adapter_down, query_up_map, key_value_up_maps, output_down_map, output_up):
    token_count = hidden.shape[0]
    group_size = HEADS // KV_HEADS
    score_scale = 1.0 / math.sqrt(HEAD_DIM)
    positions = jnp.arange(token_count, dtype=jnp.int32)
    down_flattened = adapter_down.reshape(3 * ADAPTER_RANK, MODEL_WIDTH)
    reduced_hidden = jnp.dot(hidden, down_flattened.T, preferred_element_type=jnp.float32).astype(jnp.bfloat16)
    reduced_query = reduced_hidden[:, :ADAPTER_RANK]
    reduced_key = reduced_hidden[:, ADAPTER_RANK:2 * ADAPTER_RANK]
    reduced_value = reduced_hidden[:, 2 * ADAPTER_RANK:]
    output_reduced = jnp.dot(upstream, output_up.T, preferred_element_type=jnp.float32).astype(jnp.bfloat16)
    query_projected = width_grouped(hidden, query_frozen_weight) + adapter_scale * jnp.dot(reduced_query, query_up_map, preferred_element_type=jnp.float32)
    query_states = rotate(query_projected, positions, 0, 1.0).astype(jnp.bfloat16)
    key_projected = width_grouped(hidden, key_value_frozen_weight[0]) + adapter_scale * jnp.dot(reduced_key, key_value_up_maps[0], preferred_element_type=jnp.float32)
    key_states = rotate(key_projected, positions, 0, 1.0).astype(jnp.bfloat16)
    value_state_rows = (width_grouped(hidden, key_value_frozen_weight[1]) + adapter_scale * jnp.dot(reduced_value, key_value_up_maps[1], preferred_element_type=jnp.float32)).astype(jnp.bfloat16)
    attention_output_gradient = (width_grouped(upstream, output_frozen_weight.T) + adapter_scale * jnp.dot(output_reduced, output_down_map, preferred_element_type=jnp.float32)).astype(jnp.bfloat16)
    query_heads = query_states.reshape(token_count, KV_HEADS, group_size, HEAD_DIM).transpose(1, 0, 2, 3)
    grad_heads = attention_output_gradient.reshape(token_count, KV_HEADS, group_size, HEAD_DIM).transpose(1, 0, 2, 3)
    key_heads = key_states.reshape(token_count, KV_HEADS, HEAD_DIM).transpose(1, 0, 2)
    value_heads = value_state_rows.reshape(token_count, KV_HEADS, HEAD_DIM).transpose(1, 0, 2)
    causal = positions[:, None] >= positions[None, :]

    def one_head(head_items):
        query_one = head_items[0].astype(jnp.float32)
        key_one = head_items[1].astype(jnp.float32)
        value_one = head_items[2].astype(jnp.float32)
        grad_one = head_items[3].astype(jnp.float32)
        scores = jnp.einsum('tgd,sd->gts', query_one, key_one) * score_scale
        scores = jnp.where(causal[None, :, :], scores, -jnp.inf)
        shifted = jnp.exp(scores - lax.optimization_barrier(jnp.max(scores, axis=-1, keepdims=True)))
        probs = shifted / lax.optimization_barrier(jnp.sum(shifted, axis=-1, keepdims=True))
        prob_weights = lax.optimization_barrier(probs.astype(jnp.bfloat16)).astype(jnp.float32)
        attention_one = jnp.einsum('gts,sd->tgd', prob_weights, value_one).astype(jnp.bfloat16)
        prob_grad = jnp.einsum('tgd,sd->gts', grad_one, value_one)
        delta = jnp.einsum('tgd,tgd->gt', grad_one, attention_one.astype(jnp.float32))
        score_grad = lax.optimization_barrier((probs * (prob_grad - delta[:, :, None]) * score_scale).astype(jnp.bfloat16)).astype(jnp.float32)
        query_rot = jnp.einsum('gts,sd->tgd', score_grad, key_one)
        key_rot = jnp.einsum('gts,tgd->sd', score_grad, query_one)
        value_grad = jnp.einsum('gts,tgd->sd', prob_weights, grad_one)
        return (attention_one, query_rot, key_rot, value_grad)
    attention_heads, query_rots, key_rots, value_grads = lax.map(one_head, (query_heads, key_heads, value_heads, grad_heads))
    attention_output = attention_heads.transpose(1, 0, 2, 3).reshape(token_count, HEADS * HEAD_DIM)
    query_rot_all = query_rots.transpose(1, 0, 2, 3).reshape(token_count, HEADS * HEAD_DIM)
    key_rot_all = key_rots.transpose(1, 0, 2).reshape(token_count, KV_HEADS * HEAD_DIM)
    value_all = value_grads.transpose(1, 0, 2).reshape(token_count, KV_HEADS * HEAD_DIM)
    query_rows_gradient = rotate(query_rot_all, positions, 0, -1.0).astype(jnp.bfloat16)
    key_rows_gradient = rotate(key_rot_all, positions, 0, -1.0).astype(jnp.bfloat16)
    value_rows_gradient = value_all.astype(jnp.bfloat16)
    rank_gradient = jnp.concatenate([jnp.dot(query_rows_gradient, query_up_map.T, preferred_element_type=jnp.float32), jnp.dot(key_rows_gradient, key_value_up_maps[0].T, preferred_element_type=jnp.float32), jnp.dot(value_rows_gradient, key_value_up_maps[1].T, preferred_element_type=jnp.float32)], axis=1).astype(jnp.bfloat16)
    contraction_pairs = ((query_rows_gradient, query_frozen_weight), (key_rows_gradient, key_value_frozen_weight[0]), (value_rows_gradient, key_value_frozen_weight[1]))
    hidden_gradient_total = head_grouped(contraction_pairs, token_count) + adapter_scale * jnp.dot(rank_gradient, down_flattened, preferred_element_type=jnp.float32)
    hidden_gradient = hidden_gradient_total.astype(jnp.bfloat16)
    down_map_gradient = (adapter_scale * jnp.dot(rank_gradient.T, hidden, preferred_element_type=jnp.float32)).reshape(3, ADAPTER_RANK, MODEL_WIDTH)
    query_up_map_gradient = adapter_scale * jnp.dot(reduced_query.T, query_rows_gradient, preferred_element_type=jnp.float32)
    key_value_up_maps_gradient = adapter_scale * jnp.stack([jnp.dot(reduced_key.T, key_rows_gradient, preferred_element_type=jnp.float32), jnp.dot(reduced_value.T, value_rows_gradient, preferred_element_type=jnp.float32)])
    outer_product_rank = jnp.dot(attention_output, output_down_map.T, preferred_element_type=jnp.float32).astype(jnp.bfloat16)
    output_down_map_gradient = adapter_scale * jnp.dot(output_reduced.T, attention_output, preferred_element_type=jnp.float32)
    output_up_map_gradient = adapter_scale * jnp.dot(outer_product_rank.T, upstream, preferred_element_type=jnp.float32)
    return (hidden_gradient, down_map_gradient, query_up_map_gradient, key_value_up_maps_gradient, output_down_map_gradient, output_up_map_gradient)
```

```python
import functools
import math

import jax
import jax.numpy as jnp
from jax import lax
from jax.experimental import pallas as pl
from jax.experimental.pallas import tpu as pltpu
from jax.sharding import PartitionSpec as P

KV_HEADS = 8
HEAD_DIM = 128
ADAPTER_RANK = 16
BLOCKS = 4
CHUNK_HEADS = 2
PIECES = 2


adapter_scale = 2.0
rope_base = 500000.0


def from_partner(array, axis, bit):
    return lax.ppermute(array, axis, [(i, i ^ 1 << bit) for i in range(lax.axis_size(axis))])


def rotate(values, positions, first_dim, direction):
    columns = values.shape[1]
    head_dims = (first_dim + jnp.arange(columns, dtype=jnp.int32)) % HEAD_DIM
    pair_dims = head_dims - head_dims % 2
    frequency = jnp.exp(pair_dims.astype(jnp.float32) * (-math.log(rope_base) / HEAD_DIM))
    angles = positions.astype(jnp.float32)[:, None] * frequency[None, :]
    is_even = head_dims % 2 == 0
    following = jnp.roll(values, -1, axis=1)
    preceding = jnp.roll(values, 1, axis=1)
    partner = jnp.where(is_even[None, :], -following, preceding)
    return values * jnp.cos(angles) + direction * partner * jnp.sin(angles)


def contract_last(left_side, right_side):
    return lax.dot_general(
        left_side, right_side, (((1,), (1,)), ((), ())), preferred_element_type=jnp.float32
    )


def contract_leading(left_side, right_side):
    return lax.dot_general(
        left_side, right_side, (((0,), (0,)), ((), ())), preferred_element_type=jnp.float32
    )


def shards(
    hidden,
    upstream,
    query_frozen_weight,
    key_value_frozen_weight,
    output_frozen_weight,
    adapter_down,
    query_up_map,
    key_value_up_maps,
    output_down_map,
    output_up,
):
    ffn_count = lax.axis_size("ffn")
    width_count = lax.axis_size("width")
    ffn_index = lax.axis_index("ffn")
    width_index = lax.axis_index("width")
    hidden_rows_full, upstream_gradient_full = (
        lax.all_gather(hidden, "ffn", axis=0, tiled=True),
        lax.all_gather(upstream, "ffn", axis=0, tiled=True),
    )
    token_count = hidden_rows_full.shape[0]
    query_rows = token_count // width_count
    query_cols = query_frozen_weight.shape[1]
    key_cols = key_value_frozen_weight.shape[2]
    row_start = width_index * query_rows
    positions = jnp.arange(token_count, dtype=jnp.int32)
    row_positions = row_start + jnp.arange(query_rows, dtype=jnp.int32)
    query_offset = ffn_index * query_cols
    key_offset = ffn_index * key_cols
    score_scale = 1.0 / math.sqrt(HEAD_DIM)
    down_flattened = adapter_down.reshape(3 * ADAPTER_RANK, adapter_down.shape[2])
    paired = ffn_count > KV_HEADS
    parity = ffn_index % 2
    rank_terms = contract_last(hidden_rows_full, down_flattened)
    upstream_terms = contract_last(upstream_gradient_full, output_up)
    rank_sum, upstream_sum = lax.psum((rank_terms, upstream_terms), "width")
    reduced_hidden = rank_sum.astype(jnp.bfloat16)
    output_reduced = upstream_sum.astype(jnp.bfloat16)
    low_rows = lax.dynamic_slice_in_dim(reduced_hidden, row_start, query_rows, 0)
    output_token_rows = lax.dynamic_slice_in_dim(output_reduced, row_start, query_rows, 0)
    query_part = jnp.dot(hidden_rows_full, query_frozen_weight, preferred_element_type=jnp.float32)
    query_gradient_summed = lax.psum_scatter(
        query_part.astype(jnp.bfloat16), "width", scatter_dimension=0, tiled=True
    ).astype(jnp.float32)
    query_projected = query_gradient_summed + adapter_scale * jnp.dot(
        low_rows[:, :ADAPTER_RANK], query_up_map, preferred_element_type=jnp.float32
    )
    query_states = rotate(query_projected, row_positions, query_offset, 1.0).astype(jnp.bfloat16)
    key_part = jnp.dot(
        hidden_rows_full, key_value_frozen_weight[0], preferred_element_type=jnp.float32
    )
    value_part = jnp.dot(
        hidden_rows_full, key_value_frozen_weight[1], preferred_element_type=jnp.float32
    )
    key_gradient_summed, value_gradient_summed = (
        lax.psum_scatter(
            key_part.astype(jnp.bfloat16), "width", scatter_dimension=0, tiled=True
        ).astype(jnp.float32),
        lax.psum_scatter(
            value_part.astype(jnp.bfloat16), "width", scatter_dimension=0, tiled=True
        ).astype(jnp.float32),
    )
    key_projected = key_gradient_summed + adapter_scale * jnp.dot(
        low_rows[:, ADAPTER_RANK : 2 * ADAPTER_RANK],
        key_value_up_maps[0],
        preferred_element_type=jnp.float32,
    )
    value_projected = value_gradient_summed + adapter_scale * jnp.dot(
        low_rows[:, 2 * ADAPTER_RANK :], key_value_up_maps[1], preferred_element_type=jnp.float32
    )
    key_block = rotate(key_projected, row_positions, key_offset, 1.0).astype(jnp.bfloat16)
    value_block = value_projected.astype(jnp.bfloat16)
    key_states, value_state_rows = (
        lax.all_gather(key_block, "width", axis=0, tiled=True),
        lax.all_gather(value_block, "width", axis=0, tiled=True),
    )
    if paired:
        other_key, other_value = from_partner((key_states, value_state_rows), "ffn", 0)
        key_states = jnp.where(
            parity == 0,
            jnp.concatenate([key_states, other_key], 1),
            jnp.concatenate([other_key, key_states], 1),
        )
        value_state_rows = jnp.where(
            parity == 0,
            jnp.concatenate([value_state_rows, other_value], 1),
            jnp.concatenate([other_value, value_state_rows], 1),
        )
    local_heads = query_cols // HEAD_DIM
    local_groups = key_states.shape[1] // HEAD_DIM
    group_size = local_heads // local_groups
    query_four = query_states.reshape(query_rows, local_groups, group_size, HEAD_DIM)
    key_three = key_states.reshape(token_count, local_groups, HEAD_DIM)
    value_three = value_state_rows.reshape(token_count, local_groups, HEAD_DIM)
    causal = row_positions[:, None] >= positions[None, :]
    scores = (
        jnp.einsum("qkgd,skd->kgqs", query_four, key_three, preferred_element_type=jnp.float32)
        * score_scale
    )
    scores = jnp.where(causal[None, None, :, :], scores, -jnp.inf)
    shifted = jnp.exp(scores - jnp.max(scores, axis=-1, keepdims=True))
    probs = shifted / jnp.sum(shifted, axis=-1, keepdims=True)
    prob_weights = probs.astype(jnp.bfloat16)
    attention_four = jnp.einsum(
        "kgqs,skd->qkgd", prob_weights, value_three, preferred_element_type=jnp.float32
    ).astype(jnp.bfloat16)
    attention_output = attention_four.reshape(query_rows, query_cols)
    out_part = contract_last(upstream_gradient_full, output_frozen_weight)
    output_gradient_summed = lax.psum_scatter(
        out_part.astype(jnp.bfloat16), "width", scatter_dimension=0, tiled=True
    ).astype(jnp.float32)
    attention_output_gradient = (
        output_gradient_summed
        + adapter_scale
        * jnp.dot(output_token_rows, output_down_map, preferred_element_type=jnp.float32)
    ).astype(jnp.bfloat16)
    grad_four = attention_output_gradient.reshape(query_rows, local_groups, group_size, HEAD_DIM)
    prob_grad = jnp.einsum(
        "qkgd,skd->kgqs", grad_four, value_three, preferred_element_type=jnp.float32
    )
    delta = jnp.einsum(
        "qkgd,qkgd->kgq", grad_four, attention_four, preferred_element_type=jnp.float32
    )
    score_grad = (probs * (prob_grad - delta[:, :, :, None]) * score_scale).astype(jnp.bfloat16)
    query_rot_grad = jnp.einsum(
        "kgqs,skd->qkgd", score_grad, key_three, preferred_element_type=jnp.float32
    ).reshape(query_rows, query_cols)
    key_part_grad = jnp.einsum(
        "kgqs,qkgd->skd", score_grad, query_four, preferred_element_type=jnp.float32
    ).reshape(token_count, local_groups * HEAD_DIM)
    value_part_grad = jnp.einsum(
        "kgqs,qkgd->skd", prob_weights, grad_four, preferred_element_type=jnp.float32
    ).reshape(token_count, local_groups * HEAD_DIM)
    query_block_grad = rotate(query_rot_grad, row_positions, query_offset, -1.0).astype(
        jnp.bfloat16
    )

    def own_half(values):
        return lax.dynamic_slice_in_dim(values, parity * key_cols, key_cols, 1)

    def other_half(values):
        return lax.dynamic_slice_in_dim(values, (1 - parity) * key_cols, key_cols, 1)

    key_total, value_total = lax.psum((key_part_grad, value_part_grad), "width")
    if paired:
        sent_key, sent_value = from_partner(
            (other_half(key_total), other_half(value_total)), "ffn", 0
        )
        key_total = own_half(key_total) + sent_key
        value_total = own_half(value_total) + sent_value
    key_rows_gradient = rotate(key_total, positions, key_offset, -1.0).astype(jnp.bfloat16)
    value_rows_gradient = value_total.astype(jnp.bfloat16)
    query_rows_gradient = lax.all_gather(query_block_grad, "width", axis=0, tiled=True)
    input_part = (
        contract_last(query_rows_gradient, query_frozen_weight)
        + contract_last(key_rows_gradient, key_value_frozen_weight[0])
        + contract_last(value_rows_gradient, key_value_frozen_weight[1])
    )
    rank_grad_terms = jnp.concatenate(
        [
            contract_last(query_rows_gradient, query_up_map),
            contract_last(key_rows_gradient, key_value_up_maps[0]),
            contract_last(value_rows_gradient, key_value_up_maps[1]),
        ],
        axis=1,
    )
    rank_gradient = lax.psum(rank_grad_terms, "ffn").astype(jnp.bfloat16)
    input_sum = lax.psum_scatter(
        input_part.astype(jnp.bfloat16), "ffn", scatter_dimension=0, tiled=True
    ).astype(jnp.float32)
    own_rows = token_count // ffn_count
    rank_gradient_token_rows = lax.dynamic_slice_in_dim(
        rank_gradient, ffn_index * own_rows, own_rows, 0
    )
    hidden_gradient = (
        input_sum
        + adapter_scale
        * jnp.dot(rank_gradient_token_rows, down_flattened, preferred_element_type=jnp.float32)
    ).astype(jnp.bfloat16)
    down_map_gradient = (adapter_scale * contract_leading(rank_gradient, hidden_rows_full)).reshape(
        adapter_down.shape
    )
    query_up_map_gradient = adapter_scale * contract_leading(
        reduced_hidden[:, :ADAPTER_RANK], query_rows_gradient
    )
    key_value_up_maps_gradient = adapter_scale * jnp.stack(
        [
            contract_leading(reduced_hidden[:, ADAPTER_RANK : 2 * ADAPTER_RANK], key_rows_gradient),
            contract_leading(reduced_hidden[:, 2 * ADAPTER_RANK :], value_rows_gradient),
        ]
    )
    outer_terms = contract_last(attention_output, output_down_map)
    outer_rows = lax.psum(outer_terms, "ffn").astype(jnp.bfloat16)
    outer_product_rank = lax.all_gather(outer_rows, "width", axis=0, tiled=True)
    output_down_map_gradient = adapter_scale * lax.psum(
        contract_leading(output_token_rows, attention_output), "width"
    )
    output_up_map_gradient = adapter_scale * contract_leading(
        outer_product_rank, upstream_gradient_full
    )
    return (
        hidden_gradient,
        down_map_gradient,
        query_up_map_gradient,
        key_value_up_maps_gradient,
        output_down_map_gradient,
        output_up_map_gradient,
    )


def causal_heads(scale, own_q, add_q, low, up, own_g, add_g, low_g, up_g, key, value, cosine, sine,
                 attention, query_grad, key_grad, value_grad):
    rows, columns = own_q.shape
    block = rows // BLOCKS
    even = lax.broadcasted_iota(jnp.int32, (rows, HEAD_DIM), 1) % 2 == 0
    key_all = key[...]
    value_all = value[...]
    dims_last = (((1,), (1,)), ((), ()))
    dims_first = (((0,), (0,)), ((), ()))

    def turned(values, direction):
        following = pltpu.roll(values, HEAD_DIM - 1, 1)
        preceding = pltpu.roll(values, 1, 1)
        partner = jnp.where(even, -following, preceding)
        return values * cosine[...] + direction * partner * sine[...]

    key_grad[...] = jnp.zeros_like(key_grad)
    value_grad[...] = jnp.zeros_like(value_grad)
    for head in range(columns // HEAD_DIM):
        cols = slice(head * HEAD_DIM, (head + 1) * HEAD_DIM)
        query_sum = own_q[:, cols].astype(jnp.float32) + add_q[:, cols].astype(jnp.float32)
        query_sum += adapter_scale * jnp.dot(
            low[...], up[:, cols], preferred_element_type=jnp.float32
        )
        query = turned(query_sum, 1.0).astype(jnp.bfloat16)
        grad_sum = own_g[:, cols].astype(jnp.float32) + add_g[:, cols].astype(jnp.float32)
        grad_sum += adapter_scale * jnp.dot(
            low_g[...], up_g[:, cols], preferred_element_type=jnp.float32
        )
        grad = grad_sum.astype(jnp.bfloat16)
        query_terms = []
        for index in range(BLOCKS):
            start, stop = index * block, (index + 1) * block
            query_block = query[start:stop]
            grad_block = grad[start:stop]
            key_part = key_all[:stop]
            value_part = value_all[:stop]
            scores = (
                lax.dot_general(query_block, key_part, dims_last, preferred_element_type=jnp.float32)
                * scale
            )
            row = start + lax.broadcasted_iota(jnp.int32, (block, stop), 0)
            column = lax.broadcasted_iota(jnp.int32, (block, stop), 1)
            scores = jnp.where(row >= column, scores, -jnp.inf)
            shifted = jnp.exp(scores - jnp.max(scores, axis=1, keepdims=True))
            probs = shifted * (1.0 / jnp.sum(shifted, axis=1, keepdims=True))
            weights = probs.astype(jnp.bfloat16)
            attended = jnp.dot(weights, value_part, preferred_element_type=jnp.float32).astype(
                jnp.bfloat16
            )
            attention[start:stop, cols] = attended
            prob_grad = lax.dot_general(
                grad_block, value_part, dims_last, preferred_element_type=jnp.float32
            )
            delta = jnp.sum(
                grad_block.astype(jnp.float32) * attended.astype(jnp.float32), axis=1, keepdims=True
            )
            score_grad = (probs * ((prob_grad - delta) * scale)).astype(jnp.bfloat16)
            query_terms.append(jnp.dot(score_grad, key_part, preferred_element_type=jnp.float32))
            key_grad[:stop, :] += lax.dot_general(
                score_grad, query_block, dims_first, preferred_element_type=jnp.float32
            )
            value_grad[:stop, :] += lax.dot_general(
                weights, grad_block, dims_first, preferred_element_type=jnp.float32
            )
        query_grad[:, cols] = turned(jnp.concatenate(query_terms, 0), -1.0).astype(jnp.bfloat16)


def attend(scale, *operands):
    rows, columns = operands[0].shape
    pairs = rows * rows * columns
    return pl.pallas_call(
        functools.partial(causal_heads, scale),
        out_shape=(
            jax.ShapeDtypeStruct((rows, columns), jnp.bfloat16),
            jax.ShapeDtypeStruct((rows, columns), jnp.bfloat16),
            jax.ShapeDtypeStruct((rows, HEAD_DIM), jnp.float32),
            jax.ShapeDtypeStruct((rows, HEAD_DIM), jnp.float32),
        ),
        in_specs=[pl.BlockSpec(memory_space=pltpu.VMEM)] * len(operands),
        out_specs=(pl.BlockSpec(memory_space=pltpu.VMEM),) * 4,
        compiler_params=pltpu.CompilerParams(vmem_limit_bytes=40 * 1024 * 1024),
        cost_estimate=pl.CostEstimate(
            flops=12 * pairs, bytes_accessed=16 * rows * columns, transcendentals=pairs // HEAD_DIM
        ),
    )(*operands)


def gather_tokens(block, axis):
    count = lax.axis_size(axis)
    index = lax.axis_index(axis)
    held = block
    for bit in reversed(range(count.bit_length() - 1)):
        other = from_partner(held, axis, bit)
        low_side = (index >> bit) % 2 == 0
        held = jnp.stack([jnp.where(low_side, held, other), jnp.where(low_side, other, held)])
    bits = count.bit_length() - 1
    order = tuple(reversed(range(bits))) + (bits, bits + 1)
    return held.transpose(order).reshape(count * block.shape[0], block.shape[1])


def scatter_tokens(parts, axis):
    count = lax.axis_size(axis)
    index = lax.axis_index(axis)
    bits = count.bit_length() - 1
    rows = parts.shape[0] // count
    held = parts.reshape((2,) * bits + (rows, parts.shape[1]))
    for bit in range(bits):
        dim = bits - 1 - bit
        side = (index >> bit) % 2
        mine = lax.dynamic_index_in_dim(held, side, dim, keepdims=False)
        theirs = lax.dynamic_index_in_dim(held, 1 - side, dim, keepdims=False)
        received = from_partner(theirs.astype(jnp.bfloat16), axis, bit)
        held = mine.astype(jnp.float32) + received.astype(jnp.float32)
    return held


def end_streams(
    hidden,
    upstream,
    query_frozen_weight,
    key_value_frozen_weight,
    output_frozen_weight,
    adapter_down,
    query_up_map,
    key_value_up_maps,
    output_down_map,
    output_up,
):
    ffn_count = lax.axis_size("ffn")
    width_count = lax.axis_size("width")
    ffn_index = lax.axis_index("ffn")
    width_index = lax.axis_index("width")
    last = width_count - 1
    hops = [
        [(hop, hop + 1), (last - hop, last - hop - 1)] for hop in range(last)
    ]
    is_last = width_index == last
    is_end = (width_index == 0) | is_last
    hidden_full = gather_tokens(hidden, "ffn")
    upstream_full = gather_tokens(upstream, "ffn")
    token_count = hidden_full.shape[0]
    query_cols = query_frozen_weight.shape[1]
    group_cols = query_cols // 2
    chunks = group_cols // (HEAD_DIM * CHUNK_HEADS)
    chunk_cols = group_cols // chunks
    positions = jnp.arange(token_count, dtype=jnp.int32)
    scale = 1.0 / math.sqrt(HEAD_DIM)
    down_flattened = adapter_down.reshape(3 * ADAPTER_RANK, adapter_down.shape[2])

    def to_ends(first_part, last_part):
        sent = jnp.where(width_index == 0, last_part, first_part)
        received = None
        for hop in range(last):
            if hop:
                own = jnp.where(width_index == hop, last_part, first_part)
                sent = (own.astype(jnp.float32) + received.astype(jnp.float32)).astype(jnp.bfloat16)
            received = lax.ppermute(sent, "width", hops[hop])
        return jnp.where(is_last, last_part, first_part), received

    def from_ends(own):
        first_side = own
        last_side = own
        received = own
        for hop in range(last):
            received = lax.ppermute(received, "width", hops[hop])
            first_side = jnp.where(width_index == hop + 1, received, first_side)
            last_side = jnp.where(width_index == last - 1 - hop, received, last_side)
        return first_side, last_side

    def mine(columns_of):
        half = columns_of.shape[-1] // 2
        return jnp.where(is_last, columns_of[..., half:], columns_of[..., :half])

    def product(left, right):
        return jnp.dot(left, right, preferred_element_type=jnp.float32).astype(jnp.bfloat16)

    key_value_parts = [product(hidden_full, key_value_frozen_weight[i]) for i in range(2)]
    own_kv, add_kv = to_ends(
        *[
            jnp.concatenate([part[:, side * HEAD_DIM : (side + 1) * HEAD_DIM] for part in key_value_parts], 1)
            for side in range(2)
        ]
    )
    rank_sum, upstream_sum = lax.psum(
        (contract_last(hidden_full, down_flattened), contract_last(upstream_full, output_up)), "width"
    )
    low = rank_sum.astype(jnp.bfloat16)
    out_rank = upstream_sum.astype(jnp.bfloat16)
    low_q = low[:, :ADAPTER_RANK]
    low_k = low[:, ADAPTER_RANK : 2 * ADAPTER_RANK]
    low_v = low[:, 2 * ADAPTER_RANK :]
    streams = []
    for chunk in range(chunks):
        spans = [
            slice(side * group_cols + chunk * chunk_cols, side * group_cols + (chunk + 1) * chunk_cols)
            for side in range(2)
        ]
        query_stream = to_ends(*[product(hidden_full, query_frozen_weight[:, s]) for s in spans])
        grad_stream = to_ends(
            *[contract_last(upstream_full, output_frozen_weight[s]).astype(jnp.bfloat16) for s in spans]
        )
        streams.append((query_stream, grad_stream))
    kv_sum = own_kv.astype(jnp.float32) + add_kv.astype(jnp.float32)
    key_up, value_up = mine(key_value_up_maps)
    key_state = rotate(
        kv_sum[:, :HEAD_DIM]
        + adapter_scale * jnp.dot(low_k, key_up, preferred_element_type=jnp.float32),
        positions, 0, 1.0,
    ).astype(jnp.bfloat16)
    value_state = (
        kv_sum[:, HEAD_DIM:]
        + adapter_scale * jnp.dot(low_v, value_up, preferred_element_type=jnp.float32)
    ).astype(jnp.bfloat16)
    head_dims = jnp.arange(HEAD_DIM, dtype=jnp.int32)
    frequency = jnp.exp(
        (head_dims - head_dims % 2).astype(jnp.float32) * (-math.log(rope_base) / HEAD_DIM)
    )
    angles = positions.astype(jnp.float32)[:, None] * frequency[None, :]
    cosine, sine = jnp.cos(angles), jnp.sin(angles)
    my_up = mine(query_up_map)
    my_down = mine(output_down_map)
    attentions, query_sides = [], []
    key_total = value_total = 0.0
    for chunk, ((own_q, add_q), (own_g, add_g)) in enumerate(streams):
        cols = slice(chunk * chunk_cols, (chunk + 1) * chunk_cols)
        attention, query_grad, key_term, value_term = attend(
            scale, own_q, add_q, low_q, my_up[:, cols], own_g, add_g, out_rank, my_down[:, cols],
            key_state, value_state, cosine, sine,
        )
        attentions.append(attention)
        key_total += key_term
        value_total += value_term
        query_sides.append(from_ends(query_grad))
    attention = jnp.concatenate(attentions, 1)
    key_value_grad = jnp.concatenate(
        [
            rotate(key_total, positions, 0, -1.0).astype(jnp.bfloat16),
            value_total.astype(jnp.bfloat16),
        ],
        1,
    )
    kv_sides = from_ends(key_value_grad)
    key_grad = jnp.concatenate([side[:, :HEAD_DIM] for side in kv_sides], 1)
    value_grad = jnp.concatenate([side[:, HEAD_DIM:] for side in kv_sides], 1)
    query_grad = jnp.concatenate([sides[i] for i in range(2) for sides in query_sides], 1)

    outer_terms = jnp.where(is_end, contract_last(attention, my_down), 0.0)
    outer_rank = lax.psum(outer_terms, ("ffn", "width")).astype(jnp.bfloat16)
    down_grad_part = contract_leading(out_rank, attention)
    output_down_map_gradient = adapter_scale * lax.psum(
        jnp.concatenate(
            [
                jnp.where(width_index == 0, down_grad_part, 0.0),
                jnp.where(is_last, down_grad_part, 0.0),
            ],
            1,
        ),
        "width",
    )
    output_up_map_gradient = adapter_scale * contract_leading(outer_rank, upstream_full)

    rank_terms = jnp.concatenate(
        [
            contract_last(query_grad, query_up_map),
            contract_last(key_grad, key_value_up_maps[0]),
            contract_last(value_grad, key_value_up_maps[1]),
        ],
        axis=1,
    )
    rank_gradient = lax.psum(rank_terms, "ffn").astype(jnp.bfloat16)
    input_sums = []
    out_cols = query_frozen_weight.shape[0] // PIECES
    for piece in range(PIECES):
        rows = slice(piece * out_cols, (piece + 1) * out_cols)
        total = (
            contract_last(query_grad, query_frozen_weight[rows])
            + contract_last(key_grad, key_value_frozen_weight[0, rows])
            + contract_last(value_grad, key_value_frozen_weight[1, rows])
        ).astype(jnp.bfloat16)
        input_sums.append(scatter_tokens(total, "ffn"))
    own_rows = token_count // ffn_count
    rank_rows = lax.dynamic_slice_in_dim(rank_gradient, ffn_index * own_rows, own_rows, 0)
    hidden_gradient = (
        jnp.concatenate(input_sums, 1)
        + adapter_scale * jnp.dot(rank_rows, down_flattened, preferred_element_type=jnp.float32)
    ).astype(jnp.bfloat16)
    down_map_gradient = (adapter_scale * contract_leading(rank_gradient, hidden_full)).reshape(
        adapter_down.shape
    )
    query_up_map_gradient = adapter_scale * contract_leading(low_q, query_grad)
    key_value_up_maps_gradient = adapter_scale * jnp.stack(
        [contract_leading(low_k, key_grad), contract_leading(low_v, value_grad)]
    )
    return (
        hidden_gradient,
        down_map_gradient,
        query_up_map_gradient,
        key_value_up_maps_gradient,
        output_down_map_gradient,
        output_up_map_gradient,
    )


def by_shape(*arrays):
    ffn_count = lax.axis_size("ffn")
    width_count = lax.axis_size("width")
    group_cols = arrays[2].shape[1] // 2
    fits = (
        arrays[3].shape[2] == 2 * HEAD_DIM
        and width_count % 2 == 0
        and ffn_count & (ffn_count - 1) == 0
        and group_cols % (HEAD_DIM * CHUNK_HEADS) == 0
        and (arrays[0].shape[0] * ffn_count) % (BLOCKS * HEAD_DIM) == 0
        and arrays[2].shape[0] % (PIECES * HEAD_DIM) == 0
    )
    return end_streams(*arrays) if fits else shards(*arrays)


def solution(mesh):
    placed = (
        P(("groups", "ffn"), "width"),
        P(("groups", "ffn"), "width"),
        P("width", "ffn"),
        P(None, "width", "ffn"),
        P("ffn", "width"),
        P("groups", None, "width"),
        P("groups", "ffn"),
        P("groups", None, "ffn"),
        P("groups", "ffn"),
        P("groups", "width"),
    )
    return jax.shard_map(
        by_shape,
        mesh=mesh,
        in_specs=placed,
        out_specs=(
            P(("groups", "ffn"), "width"),
            P("groups", None, "width"),
            P("groups", "ffn"),
            P("groups", None, "ffn"),
            P("groups", "ffn"),
            P("groups", "width"),
        ),
        check_vma=False,
    )
```

```python
import functools
import math

import jax
import jax.numpy as jnp
from jax import lax
from jax.experimental import pallas as pl
from jax.experimental.pallas import tpu as pltpu
from jax.sharding import PartitionSpec as P

KV_HEADS = 8
HEAD_DIM = 128
ADAPTER_RANK = 16
BLOCKS = 4
CHUNK_HEADS = 2
PIECES = 2


adapter_scale = 2.0
rope_base = 500000.0


def from_partner(array, axis, bit):
    return lax.ppermute(array, axis, [(i, i ^ 1 << bit) for i in range(lax.axis_size(axis))])


def rotate(values, positions, first_dim, direction):
    columns = values.shape[1]
    head_dims = (first_dim + jnp.arange(columns, dtype=jnp.int32)) % HEAD_DIM
    pair_dims = head_dims - head_dims % 2
    frequency = jnp.exp(pair_dims.astype(jnp.float32) * (-math.log(rope_base) / HEAD_DIM))
    angles = positions.astype(jnp.float32)[:, None] * frequency[None, :]
    is_even = head_dims % 2 == 0
    following = jnp.roll(values, -1, axis=1)
    preceding = jnp.roll(values, 1, axis=1)
    partner = jnp.where(is_even[None, :], -following, preceding)
    return values * jnp.cos(angles) + direction * partner * jnp.sin(angles)


def contract_last(left_side, right_side):
    return lax.dot_general(
        left_side, right_side, (((1,), (1,)), ((), ())), preferred_element_type=jnp.float32
    )


def contract_leading(left_side, right_side):
    return lax.dot_general(
        left_side, right_side, (((0,), (0,)), ((), ())), preferred_element_type=jnp.float32
    )


def shards(
    hidden,
    upstream,
    query_frozen_weight,
    key_value_frozen_weight,
    output_frozen_weight,
    adapter_down,
    query_up_map,
    key_value_up_maps,
    output_down_map,
    output_up,
):
    ffn_count = lax.axis_size("ffn")
    width_count = lax.axis_size("width")
    ffn_index = lax.axis_index("ffn")
    width_index = lax.axis_index("width")
    hidden_rows_full, upstream_gradient_full = (
        lax.all_gather(hidden, "ffn", axis=0, tiled=True),
        lax.all_gather(upstream, "ffn", axis=0, tiled=True),
    )
    token_count = hidden_rows_full.shape[0]
    query_rows = token_count // width_count
    query_cols = query_frozen_weight.shape[1]
    key_cols = key_value_frozen_weight.shape[2]
    row_start = width_index * query_rows
    positions = jnp.arange(token_count, dtype=jnp.int32)
    row_positions = row_start + jnp.arange(query_rows, dtype=jnp.int32)
    query_offset = ffn_index * query_cols
    key_offset = ffn_index * key_cols
    score_scale = 1.0 / math.sqrt(HEAD_DIM)
    down_flattened = adapter_down.reshape(3 * ADAPTER_RANK, adapter_down.shape[2])
    paired = ffn_count > KV_HEADS
    parity = ffn_index % 2
    rank_terms = contract_last(hidden_rows_full, down_flattened)
    upstream_terms = contract_last(upstream_gradient_full, output_up)
    rank_sum, upstream_sum = lax.psum((rank_terms, upstream_terms), "width")
    reduced_hidden = rank_sum.astype(jnp.bfloat16)
    output_reduced = upstream_sum.astype(jnp.bfloat16)
    low_rows = lax.dynamic_slice_in_dim(reduced_hidden, row_start, query_rows, 0)
    output_token_rows = lax.dynamic_slice_in_dim(output_reduced, row_start, query_rows, 0)
    query_part = jnp.dot(hidden_rows_full, query_frozen_weight, preferred_element_type=jnp.float32)
    query_gradient_summed = lax.psum_scatter(
        query_part.astype(jnp.bfloat16), "width", scatter_dimension=0, tiled=True
    ).astype(jnp.float32)
    query_projected = query_gradient_summed + adapter_scale * jnp.dot(
        low_rows[:, :ADAPTER_RANK], query_up_map, preferred_element_type=jnp.float32
    )
    query_states = rotate(query_projected, row_positions, query_offset, 1.0).astype(jnp.bfloat16)
    key_part = jnp.dot(
        hidden_rows_full, key_value_frozen_weight[0], preferred_element_type=jnp.float32
    )
    value_part = jnp.dot(
        hidden_rows_full, key_value_frozen_weight[1], preferred_element_type=jnp.float32
    )
    key_gradient_summed, value_gradient_summed = (
        lax.psum_scatter(
            key_part.astype(jnp.bfloat16), "width", scatter_dimension=0, tiled=True
        ).astype(jnp.float32),
        lax.psum_scatter(
            value_part.astype(jnp.bfloat16), "width", scatter_dimension=0, tiled=True
        ).astype(jnp.float32),
    )
    key_projected = key_gradient_summed + adapter_scale * jnp.dot(
        low_rows[:, ADAPTER_RANK : 2 * ADAPTER_RANK],
        key_value_up_maps[0],
        preferred_element_type=jnp.float32,
    )
    value_projected = value_gradient_summed + adapter_scale * jnp.dot(
        low_rows[:, 2 * ADAPTER_RANK :], key_value_up_maps[1], preferred_element_type=jnp.float32
    )
    key_block = rotate(key_projected, row_positions, key_offset, 1.0).astype(jnp.bfloat16)
    value_block = value_projected.astype(jnp.bfloat16)
    key_states, value_state_rows = (
        lax.all_gather(key_block, "width", axis=0, tiled=True),
        lax.all_gather(value_block, "width", axis=0, tiled=True),
    )
    if paired:
        other_key, other_value = from_partner((key_states, value_state_rows), "ffn", 0)
        key_states = jnp.where(
            parity == 0,
            jnp.concatenate([key_states, other_key], 1),
            jnp.concatenate([other_key, key_states], 1),
        )
        value_state_rows = jnp.where(
            parity == 0,
            jnp.concatenate([value_state_rows, other_value], 1),
            jnp.concatenate([other_value, value_state_rows], 1),
        )
    local_heads = query_cols // HEAD_DIM
    local_groups = key_states.shape[1] // HEAD_DIM
    group_size = local_heads // local_groups
    query_four = query_states.reshape(query_rows, local_groups, group_size, HEAD_DIM)
    key_three = key_states.reshape(token_count, local_groups, HEAD_DIM)
    value_three = value_state_rows.reshape(token_count, local_groups, HEAD_DIM)
    causal = row_positions[:, None] >= positions[None, :]
    scores = (
        jnp.einsum("qkgd,skd->kgqs", query_four, key_three, preferred_element_type=jnp.float32)
        * score_scale
    )
    scores = jnp.where(causal[None, None, :, :], scores, -jnp.inf)
    shifted = jnp.exp(scores - jnp.max(scores, axis=-1, keepdims=True))
    probs = shifted / jnp.sum(shifted, axis=-1, keepdims=True)
    prob_weights = probs.astype(jnp.bfloat16)
    attention_four = jnp.einsum(
        "kgqs,skd->qkgd", prob_weights, value_three, preferred_element_type=jnp.float32
    ).astype(jnp.bfloat16)
    attention_output = attention_four.reshape(query_rows, query_cols)
    out_part = contract_last(upstream_gradient_full, output_frozen_weight)
    output_gradient_summed = lax.psum_scatter(
        out_part.astype(jnp.bfloat16), "width", scatter_dimension=0, tiled=True
    ).astype(jnp.float32)
    attention_output_gradient = (
        output_gradient_summed
        + adapter_scale
        * jnp.dot(output_token_rows, output_down_map, preferred_element_type=jnp.float32)
    ).astype(jnp.bfloat16)
    grad_four = attention_output_gradient.reshape(query_rows, local_groups, group_size, HEAD_DIM)
    prob_grad = jnp.einsum(
        "qkgd,skd->kgqs", grad_four, value_three, preferred_element_type=jnp.float32
    )
    delta = jnp.einsum(
        "qkgd,qkgd->kgq", grad_four, attention_four, preferred_element_type=jnp.float32
    )
    score_grad = (probs * (prob_grad - delta[:, :, :, None]) * score_scale).astype(jnp.bfloat16)
    query_rot_grad = jnp.einsum(
        "kgqs,skd->qkgd", score_grad, key_three, preferred_element_type=jnp.float32
    ).reshape(query_rows, query_cols)
    key_part_grad = jnp.einsum(
        "kgqs,qkgd->skd", score_grad, query_four, preferred_element_type=jnp.float32
    ).reshape(token_count, local_groups * HEAD_DIM)
    value_part_grad = jnp.einsum(
        "kgqs,qkgd->skd", prob_weights, grad_four, preferred_element_type=jnp.float32
    ).reshape(token_count, local_groups * HEAD_DIM)
    query_block_grad = rotate(query_rot_grad, row_positions, query_offset, -1.0).astype(
        jnp.bfloat16
    )

    def own_half(values):
        return lax.dynamic_slice_in_dim(values, parity * key_cols, key_cols, 1)

    def other_half(values):
        return lax.dynamic_slice_in_dim(values, (1 - parity) * key_cols, key_cols, 1)

    key_total, value_total = lax.psum((key_part_grad, value_part_grad), "width")
    if paired:
        sent_key, sent_value = from_partner(
            (other_half(key_total), other_half(value_total)), "ffn", 0
        )
        key_total = own_half(key_total) + sent_key
        value_total = own_half(value_total) + sent_value
    key_rows_gradient = rotate(key_total, positions, key_offset, -1.0).astype(jnp.bfloat16)
    value_rows_gradient = value_total.astype(jnp.bfloat16)
    query_rows_gradient = lax.all_gather(query_block_grad, "width", axis=0, tiled=True)
    input_part = (
        contract_last(query_rows_gradient, query_frozen_weight)
        + contract_last(key_rows_gradient, key_value_frozen_weight[0])
        + contract_last(value_rows_gradient, key_value_frozen_weight[1])
    )
    rank_grad_terms = jnp.concatenate(
        [
            contract_last(query_rows_gradient, query_up_map),
            contract_last(key_rows_gradient, key_value_up_maps[0]),
            contract_last(value_rows_gradient, key_value_up_maps[1]),
        ],
        axis=1,
    )
    rank_gradient = lax.psum(rank_grad_terms, "ffn").astype(jnp.bfloat16)
    input_sum = lax.psum_scatter(
        input_part.astype(jnp.bfloat16), "ffn", scatter_dimension=0, tiled=True
    ).astype(jnp.float32)
    own_rows = token_count // ffn_count
    rank_gradient_token_rows = lax.dynamic_slice_in_dim(
        rank_gradient, ffn_index * own_rows, own_rows, 0
    )
    hidden_gradient = (
        input_sum
        + adapter_scale
        * jnp.dot(rank_gradient_token_rows, down_flattened, preferred_element_type=jnp.float32)
    ).astype(jnp.bfloat16)
    down_map_gradient = (adapter_scale * contract_leading(rank_gradient, hidden_rows_full)).reshape(
        adapter_down.shape
    )
    query_up_map_gradient = adapter_scale * contract_leading(
        reduced_hidden[:, :ADAPTER_RANK], query_rows_gradient
    )
    key_value_up_maps_gradient = adapter_scale * jnp.stack(
        [
            contract_leading(reduced_hidden[:, ADAPTER_RANK : 2 * ADAPTER_RANK], key_rows_gradient),
            contract_leading(reduced_hidden[:, 2 * ADAPTER_RANK :], value_rows_gradient),
        ]
    )
    outer_terms = contract_last(attention_output, output_down_map)
    outer_rows = lax.psum(outer_terms, "ffn").astype(jnp.bfloat16)
    outer_product_rank = lax.all_gather(outer_rows, "width", axis=0, tiled=True)
    output_down_map_gradient = adapter_scale * lax.psum(
        contract_leading(output_token_rows, attention_output), "width"
    )
    output_up_map_gradient = adapter_scale * contract_leading(
        outer_product_rank, upstream_gradient_full
    )
    return (
        hidden_gradient,
        down_map_gradient,
        query_up_map_gradient,
        key_value_up_maps_gradient,
        output_down_map_gradient,
        output_up_map_gradient,
    )


def causal_heads(scale, own_q, add_q, low, up, own_g, add_g, low_g, up_g, key, value, cosine, sine,
                 attention, query_grad, key_grad, value_grad):
    rows, columns = own_q.shape
    block = rows // BLOCKS
    even = lax.broadcasted_iota(jnp.int32, (rows, HEAD_DIM), 1) % 2 == 0
    key_all = key[...]
    value_all = value[...]
    dims_last = (((1,), (1,)), ((), ()))
    dims_first = (((0,), (0,)), ((), ()))

    def turned(values, direction):
        following = pltpu.roll(values, HEAD_DIM - 1, 1)
        preceding = pltpu.roll(values, 1, 1)
        partner = jnp.where(even, -following, preceding)
        return values * cosine[...] + direction * partner * sine[...]

    key_grad[...] = jnp.zeros_like(key_grad)
    value_grad[...] = jnp.zeros_like(value_grad)
    for head in range(columns // HEAD_DIM):
        cols = slice(head * HEAD_DIM, (head + 1) * HEAD_DIM)
        query_sum = own_q[:, cols].astype(jnp.float32) + add_q[:, cols].astype(jnp.float32)
        query_sum += adapter_scale * jnp.dot(
            low[...], up[:, cols], preferred_element_type=jnp.float32
        )
        query = turned(query_sum, 1.0).astype(jnp.bfloat16)
        grad_sum = own_g[:, cols].astype(jnp.float32) + add_g[:, cols].astype(jnp.float32)
        grad_sum += adapter_scale * jnp.dot(
            low_g[...], up_g[:, cols], preferred_element_type=jnp.float32
        )
        grad = grad_sum.astype(jnp.bfloat16)
        query_terms = []
        for index in range(BLOCKS):
            start, stop = index * block, (index + 1) * block
            query_block = query[start:stop]
            grad_block = grad[start:stop]
            key_part = key_all[:stop]
            value_part = value_all[:stop]
            scores = (
                lax.dot_general(query_block, key_part, dims_last, preferred_element_type=jnp.float32)
                * scale
            )
            row = start + lax.broadcasted_iota(jnp.int32, (block, stop), 0)
            column = lax.broadcasted_iota(jnp.int32, (block, stop), 1)
            scores = jnp.where(row >= column, scores, -jnp.inf)
            shifted = jnp.exp(scores - jnp.max(scores, axis=1, keepdims=True))
            probs = shifted * (1.0 / jnp.sum(shifted, axis=1, keepdims=True))
            weights = probs.astype(jnp.bfloat16)
            attended = jnp.dot(weights, value_part, preferred_element_type=jnp.float32).astype(
                jnp.bfloat16
            )
            attention[start:stop, cols] = attended
            prob_grad = lax.dot_general(
                grad_block, value_part, dims_last, preferred_element_type=jnp.float32
            )
            delta = jnp.sum(
                grad_block.astype(jnp.float32) * attended.astype(jnp.float32), axis=1, keepdims=True
            )
            score_grad = (probs * ((prob_grad - delta) * scale)).astype(jnp.bfloat16)
            query_terms.append(jnp.dot(score_grad, key_part, preferred_element_type=jnp.float32))
            key_grad[:stop, :] += lax.dot_general(
                score_grad, query_block, dims_first, preferred_element_type=jnp.float32
            )
            value_grad[:stop, :] += lax.dot_general(
                weights, grad_block, dims_first, preferred_element_type=jnp.float32
            )
        query_grad[:, cols] = turned(jnp.concatenate(query_terms, 0), -1.0).astype(jnp.bfloat16)


def attend(scale, *operands):
    rows, columns = operands[0].shape
    pairs = rows * rows * columns
    return pl.pallas_call(
        functools.partial(causal_heads, scale),
        out_shape=(
            jax.ShapeDtypeStruct((rows, columns), jnp.bfloat16),
            jax.ShapeDtypeStruct((rows, columns), jnp.bfloat16),
            jax.ShapeDtypeStruct((rows, HEAD_DIM), jnp.float32),
            jax.ShapeDtypeStruct((rows, HEAD_DIM), jnp.float32),
        ),
        in_specs=[pl.BlockSpec(memory_space=pltpu.VMEM)] * len(operands),
        out_specs=(pl.BlockSpec(memory_space=pltpu.VMEM),) * 4,
        compiler_params=pltpu.CompilerParams(vmem_limit_bytes=40 * 1024 * 1024),
        cost_estimate=pl.CostEstimate(
            flops=12 * pairs, bytes_accessed=16 * rows * columns, transcendentals=pairs // HEAD_DIM
        ),
    )(*operands)


def pair_sum(values, axis):
    for bit in range(lax.axis_size(axis).bit_length() - 1):
        values = values + from_partner(values, axis, bit)
    return values


def scatter_tokens(parts, axis):
    count = lax.axis_size(axis)
    index = lax.axis_index(axis)
    bits = count.bit_length() - 1
    rows = parts.shape[0] // count
    held = parts.reshape((2,) * bits + (rows, parts.shape[1]))
    for bit in range(bits):
        dim = bits - 1 - bit
        side = (index >> bit) % 2
        mine = lax.dynamic_index_in_dim(held, side, dim, keepdims=False)
        theirs = lax.dynamic_index_in_dim(held, 1 - side, dim, keepdims=False)
        received = from_partner(theirs.astype(jnp.bfloat16), axis, bit)
        held = mine.astype(jnp.float32) + received.astype(jnp.float32)
    return held


def end_streams(
    hidden,
    upstream,
    query_frozen_weight,
    key_value_frozen_weight,
    output_frozen_weight,
    adapter_down,
    query_up_map,
    key_value_up_maps,
    output_down_map,
    output_up,
):
    ffn_count = lax.axis_size("ffn")
    width_count = lax.axis_size("width")
    ffn_index = lax.axis_index("ffn")
    width_index = lax.axis_index("width")
    last = width_count - 1
    hops = [
        [(hop, hop + 1), (last - hop, last - hop - 1)] for hop in range(last)
    ]
    is_last = width_index == last
    is_end = (width_index == 0) | is_last
    hidden_full = lax.all_gather(hidden, "ffn", axis=0, tiled=True)
    upstream, hidden_full = lax.optimization_barrier((upstream, hidden_full))
    upstream_full = lax.all_gather(upstream, "ffn", axis=0, tiled=True)
    token_count = hidden_full.shape[0]
    query_cols = query_frozen_weight.shape[1]
    group_cols = query_cols // 2
    chunks = group_cols // (HEAD_DIM * CHUNK_HEADS)
    chunk_cols = group_cols // chunks
    positions = jnp.arange(token_count, dtype=jnp.int32)
    scale = 1.0 / math.sqrt(HEAD_DIM)
    down_flattened = adapter_down.reshape(3 * ADAPTER_RANK, adapter_down.shape[2])

    def to_ends(first_part, last_part):
        sent = jnp.where(width_index == 0, last_part, first_part)
        received = None
        for hop in range(last):
            if hop:
                own = jnp.where(width_index == hop, last_part, first_part)
                sent = (own.astype(jnp.float32) + received.astype(jnp.float32)).astype(jnp.bfloat16)
            received = lax.ppermute(sent, "width", hops[hop])
        return jnp.where(is_last, last_part, first_part), received

    first_hops = []

    def line_sum(own):
        total = own.astype(jnp.float32)
        received = None
        for hop in range(last):
            sent = own if hop == 0 else own + received
            received = lax.ppermute(sent, "width", hops[hop])
            total = total + received.astype(jnp.float32)
        return total

    def from_ends(own):
        first_side = own
        last_side = own
        received = own
        for hop in range(last):
            received = lax.ppermute(received, "width", hops[hop])
            if hop == 0:
                first_hops.append(received)
            first_side = jnp.where(width_index == hop + 1, received, first_side)
            last_side = jnp.where(width_index == last - 1 - hop, received, last_side)
        return first_side, last_side

    def mine(columns_of):
        half = columns_of.shape[-1] // 2
        return jnp.where(is_last, columns_of[..., half:], columns_of[..., :half])

    def product(left, right):
        return jnp.dot(left, right, preferred_element_type=jnp.float32).astype(jnp.bfloat16)

    key_value_parts = [product(hidden_full, key_value_frozen_weight[i]) for i in range(2)]
    own_kv, add_kv = to_ends(
        *[
            jnp.concatenate([part[:, side * HEAD_DIM : (side + 1) * HEAD_DIM] for part in key_value_parts], 1)
            for side in range(2)
        ]
    )
    low = line_sum(contract_last(down_flattened, hidden_full).astype(jnp.bfloat16))
    low = low.astype(jnp.bfloat16).T
    out_rank = line_sum(contract_last(output_up, upstream_full).astype(jnp.bfloat16))
    out_rank = out_rank.astype(jnp.bfloat16).T
    low_q = low[:, :ADAPTER_RANK]
    low_k = low[:, ADAPTER_RANK : 2 * ADAPTER_RANK]
    low_v = low[:, 2 * ADAPTER_RANK :]
    streams = []
    for chunk in range(chunks):
        spans = [
            slice(side * group_cols + chunk * chunk_cols, side * group_cols + (chunk + 1) * chunk_cols)
            for side in range(2)
        ]
        query_stream = to_ends(*[product(hidden_full, query_frozen_weight[:, s]) for s in spans])
        grad_stream = to_ends(
            *[contract_last(upstream_full, output_frozen_weight[s]).astype(jnp.bfloat16) for s in spans]
        )
        streams.append((query_stream, grad_stream))
    kv_sum = own_kv.astype(jnp.float32) + add_kv.astype(jnp.float32)
    key_up, value_up = mine(key_value_up_maps)
    key_state = rotate(
        kv_sum[:, :HEAD_DIM]
        + adapter_scale * jnp.dot(low_k, key_up, preferred_element_type=jnp.float32),
        positions, 0, 1.0,
    ).astype(jnp.bfloat16)
    value_state = (
        kv_sum[:, HEAD_DIM:]
        + adapter_scale * jnp.dot(low_v, value_up, preferred_element_type=jnp.float32)
    ).astype(jnp.bfloat16)
    head_dims = jnp.arange(HEAD_DIM, dtype=jnp.int32)
    frequency = jnp.exp(
        (head_dims - head_dims % 2).astype(jnp.float32) * (-math.log(rope_base) / HEAD_DIM)
    )
    angles = positions.astype(jnp.float32)[:, None] * frequency[None, :]
    cosine, sine = jnp.cos(angles), jnp.sin(angles)
    my_up = mine(query_up_map)
    my_down = mine(output_down_map)
    attentions, query_sides = [], []
    key_total = value_total = 0.0
    for chunk, ((own_q, add_q), (own_g, add_g)) in enumerate(streams):
        cols = slice(chunk * chunk_cols, (chunk + 1) * chunk_cols)
        if chunk > 1:
            add_q, first_hops[chunk - 2] = lax.optimization_barrier((add_q, first_hops[chunk - 2]))
        attention, query_grad, key_term, value_term = attend(
            scale, own_q, add_q, low_q, my_up[:, cols], own_g, add_g, out_rank, my_down[:, cols],
            key_state, value_state, cosine, sine,
        )
        attentions.append(attention)
        key_total += key_term
        value_total += value_term
        query_sides.append(from_ends(query_grad))
    attention = jnp.concatenate(attentions, 1)
    key_value_grad = jnp.concatenate(
        [
            rotate(key_total, positions, 0, -1.0).astype(jnp.bfloat16),
            value_total.astype(jnp.bfloat16),
        ],
        1,
    )
    kv_sides = from_ends(key_value_grad)
    key_grad = jnp.concatenate([side[:, :HEAD_DIM] for side in kv_sides], 1)
    value_grad = jnp.concatenate([side[:, HEAD_DIM:] for side in kv_sides], 1)
    query_grad = jnp.concatenate([sides[i] for i in range(2) for sides in query_sides], 1)

    outer_terms = jnp.where(is_end, contract_last(my_down, attention), 0.0)
    outer_rank = pair_sum(line_sum(outer_terms), "ffn").astype(jnp.bfloat16).T
    output_down_map_gradient = adapter_scale * jnp.concatenate(
        from_ends(contract_leading(out_rank, attention)), 1
    )
    output_up_map_gradient = adapter_scale * contract_leading(outer_rank, upstream_full)

    rank_terms = jnp.concatenate(
        [
            contract_last(query_up_map, query_grad),
            contract_last(key_value_up_maps[0], key_grad),
            contract_last(key_value_up_maps[1], value_grad),
        ],
        axis=0,
    )
    rank_gradient = pair_sum(rank_terms, "ffn").astype(jnp.bfloat16).T
    input_sums = []
    out_cols = query_frozen_weight.shape[0] // PIECES
    for piece in range(PIECES):
        rows = slice(piece * out_cols, (piece + 1) * out_cols)
        total = (
            contract_last(query_grad, query_frozen_weight[rows])
            + contract_last(key_grad, key_value_frozen_weight[0, rows])
            + contract_last(value_grad, key_value_frozen_weight[1, rows])
        ).astype(jnp.bfloat16)
        input_sums.append(scatter_tokens(total, "ffn"))
    own_rows = token_count // ffn_count
    rank_rows = lax.dynamic_slice_in_dim(rank_gradient, ffn_index * own_rows, own_rows, 0)
    hidden_gradient = (
        jnp.concatenate(input_sums, 1)
        + adapter_scale * jnp.dot(rank_rows, down_flattened, preferred_element_type=jnp.float32)
    ).astype(jnp.bfloat16)
    down_map_gradient = (adapter_scale * contract_leading(rank_gradient, hidden_full)).reshape(
        adapter_down.shape
    )
    query_up_map_gradient = adapter_scale * contract_leading(low_q, query_grad)
    key_value_up_maps_gradient = adapter_scale * jnp.stack(
        [contract_leading(low_k, key_grad), contract_leading(low_v, value_grad)]
    )
    return (
        hidden_gradient,
        down_map_gradient,
        query_up_map_gradient,
        key_value_up_maps_gradient,
        output_down_map_gradient,
        output_up_map_gradient,
    )


def by_shape(*arrays):
    ffn_count = lax.axis_size("ffn")
    width_count = lax.axis_size("width")
    group_cols = arrays[2].shape[1] // 2
    fits = (
        arrays[3].shape[2] == 2 * HEAD_DIM
        and width_count % 2 == 0
        and ffn_count & (ffn_count - 1) == 0
        and group_cols % (HEAD_DIM * CHUNK_HEADS) == 0
        and (arrays[0].shape[0] * ffn_count) % (BLOCKS * HEAD_DIM) == 0
        and arrays[2].shape[0] % (PIECES * HEAD_DIM) == 0
    )
    return end_streams(*arrays) if fits else shards(*arrays)


def solution(mesh):
    placed = (
        P(("groups", "ffn"), "width"),
        P(("groups", "ffn"), "width"),
        P("width", "ffn"),
        P(None, "width", "ffn"),
        P("ffn", "width"),
        P("groups", None, "width"),
        P("groups", "ffn"),
        P("groups", None, "ffn"),
        P("groups", "ffn"),
        P("groups", "width"),
    )
    return jax.shard_map(
        by_shape,
        mesh=mesh,
        in_specs=placed,
        out_specs=(
            P(("groups", "ffn"), "width"),
            P("groups", None, "width"),
            P("groups", "ffn"),
            P("groups", None, "ffn"),
            P("groups", "ffn"),
            P("groups", "width"),
        ),
        check_vma=False,
    )
```
